32 devices in a mesh: replica: 8 (over y, x, core), tensor: 4 (over z).
Axes of the slice: x: 2, y: 2, z: 4, core: 2. Of those that a mesh axis runs over, the one named last changes fastest.
Arguments:
- weights: bfloat16 [8, 7168, 2048], P('replica', 'tensor'), may hold values from -6 to 6
- hidden: bfloat16 [8, 2, 512, 7168], P('replica', None, None, 'tensor'), may hold values from -6 to 6
- targets: bfloat16 [8, 2, 512, 2048], P('replica'), may hold values from -6 to 6
- norm_gain: float32 [2048], replicated, may hold values from 0.5 to 2
- stragglers: int32 [2, 8], replicated, may hold values 0 or 1
Outputs:
- new_weights: bfloat16 [8, 7168, 2048], P('replica', 'tensor')
The draws below stay inside these ranges and needn't reach their ends.
All inputs are finite; a program needn't handle non-finite values.
Results may differ from the reference program's by a relative error of at most 0.011.
Values may be sent and summed in bfloat16 or wider, within the bound.
A program may use at most 128 MiB of HBM per device.

```python
import math
import jax
import jax.numpy as jnp
from jax import lax

D = 2048
FF = 7168
TOK_DEV = 512
STEPS = 2
REPLICAS = 8
N_REPLICA = 8


def set_ends(entries, own_key, low, high):
    place = [jax.random.randint(jax.random.fold_in(own_key, axis), (), 0, length) for axis, length in enumerate(entries.shape)]
    widest = entries.shape.index(max(entries.shape))
    neighbour = place[:widest] + [(place[widest] + 1) % entries.shape[widest]] + place[widest + 1:]
    return entries.at[tuple(place)].set(low).at[tuple(neighbour)].set(high)


def block_levels(key, dims, shards, smallest, top_value):
    loudness, own = 1.0, jax.random.fold_in(key, 6)
    for position, blocks in shards:
        heights = jnp.exp(jax.random.uniform(jax.random.fold_in(own, position), (blocks,), jnp.float32, smallest / len(shards), top_value / len(shards)))
        loudness = loudness * jnp.repeat(heights, dims[position] // blocks).reshape([-1 if axis == position else 1 for axis in range(len(dims))])
    return loudness


def centred(rng, dims, spread, most, shards=(), held_as=jnp.bfloat16):
    factor_of = block_levels(rng, dims, shards, -0.22, 0.18) if shards else 1.0
    drawn = jax.random.normal(rng, dims, jnp.float32) * spread * factor_of
    return jnp.minimum(jnp.maximum(drawn, -most), most).astype(held_as)


def setup_inputs(seed: int = 0) -> dict:
    arg_keys = jax.random.split(jax.random.key(seed), 6)
    return {
        "weights": centred(arg_keys[0], (REPLICAS, FF, D), 1.0, 6.0, ((0, 8), (1, 4))),
        "hidden": centred(arg_keys[1], (REPLICAS, STEPS, TOK_DEV, FF), 1.0, 6.0, ((0, 8), (3, 4))),
        "targets": centred(arg_keys[2], (REPLICAS, STEPS, TOK_DEV, D), 1.0, 6.0, ((0, 8),)),
        "norm_gain": jnp.clip(jnp.exp(jax.random.uniform(arg_keys[3], (D,), jnp.float32, math.log(0.5), math.log(2.0))), 0.5, 2.0),
        "stragglers": set_ends((jax.random.randint(arg_keys[4], (STEPS, REPLICAS), 0, 4) < 1).astype(jnp.int32), jax.random.fold_in(arg_keys[4], 1), 0, 1),
    }


eps = 1e-05
learn_rate = 0.5

def contract_rows(left, right):
    return lax.dot_general(left, right, (((0,), (0,)), ((), ())), preferred_element_type=jnp.float32)

def norm_backward(outputs, target_rows, norm_gain):
    squares = lax.optimization_barrier(jnp.mean(outputs * outputs, axis=-1, keepdims=True))
    inverse = lax.rsqrt(squares + eps)
    normed = outputs * inverse
    weighted = (normed * norm_gain - target_rows.astype(jnp.float32)) * norm_gain
    cross_mean = lax.optimization_barrier(jnp.mean(weighted * normed, axis=-1, keepdims=True))
    return (inverse * (weighted - normed * cross_mean)).astype(jnp.bfloat16)

def local_update(weight_block, hidden_rows, target_rows, norm_gain):
    factor = FF ** (-0.5)
    outputs = factor * jnp.dot(hidden_rows, weight_block, preferred_element_type=jnp.float32)
    grad_out = norm_backward(outputs, target_rows, norm_gain)
    grad_weight = (factor * contract_rows(hidden_rows, grad_out)).astype(jnp.bfloat16)
    return (weight_block.astype(jnp.float32) - learn_rate * grad_weight.astype(jnp.float32)).astype(jnp.bfloat16)

def reference(weights, hidden, targets, norm_gain, stragglers):
    levels = N_REPLICA.bit_length() - 1
    indices = jnp.arange(N_REPLICA, dtype=jnp.int32)
    for update_step in range(STEPS):
        bit_index = update_step % levels
        updated = lax.map(lambda element: local_update(element[0], element[1], element[2], norm_gain), (weights, hidden[:, update_step], targets[:, update_step]))
        partner = jnp.bitwise_xor(indices, jnp.int32(1 << bit_index)).astype(jnp.int32)
        paired = updated[partner]
        mask_row = stragglers[update_step]
        keep_pair = (mask_row == 0) & (mask_row[partner] == 0)
        averaged = ((updated.astype(jnp.float32) + paired.astype(jnp.float32)) * 0.5).astype(jnp.bfloat16)
        weights = jnp.where(keep_pair[:, None, None], averaged, updated)
    return weights
```

```python
import functools

import jax
import jax.numpy as jnp
from jax import lax
from jax.experimental import pallas as pl
from jax.experimental.pallas import tpu as pltpu
from jax.sharding import PartitionSpec as P

FF = 7168
STEPS = 2


eps = 1e-05
learn_rate = 0.5

MESH = pl.DeviceIdType.MESH
TILE = 256
ROWS = 256
PIECES = 16
AHEAD = 2
BESIDE = 6


def partner(block, axis, apart):
    count = lax.axis_size(axis)
    route = []
    for low in range(count):
        high = low | 1 << apart
        if high != low and high < count:
            route += [(low, high), (high, low)]
    return lax.ppermute(block, axis, route)


def contract_rows(left, right):
    return lax.dot_general(
        left, right, (((0,), (0,)), ((), ())), preferred_element_type=jnp.float32
    )


def norm_backward(outputs, target_rows, norm_gain):
    squares = jnp.mean(outputs * outputs, axis=-1, keepdims=True)
    inverse = lax.rsqrt(squares + eps)
    normed = outputs * inverse
    weighted = (normed * norm_gain - target_rows.astype(jnp.float32)) * norm_gain
    cross_mean = jnp.mean(weighted * normed, axis=-1, keepdims=True)
    return (inverse * (weighted - normed * cross_mean)).astype(jnp.bfloat16)


def descend(weight_block, hidden_rows, grad_out):
    factor = FF ** (-0.5)
    grad_weight = (factor * contract_rows(hidden_rows, grad_out)).astype(jnp.bfloat16)
    return (
        weight_block.astype(jnp.float32) - learn_rate * grad_weight.astype(jnp.float32)
    ).astype(jnp.bfloat16)


def step_kernel(apart, last, *refs):
    hidden_ref, weight_ref, target_ref, gain_ref, cargo_ref = refs[:5]
    if last:
        grad_ref, landed_ref, paired_ref = refs[5:8]
        rest = refs[8:]
    else:
        grad_ref, landed_ref = refs[5:7]
        rest = refs[7:]
    terms, in_right, in_left, out_right, out_left = rest[:5]
    right_send, right_recv, left_send, left_recv, cargo_send, cargo_recv = rest[5:11]
    if last:
        far_grad, grad_send, grad_recv, share_send, share_recv = rest[11:]

    count = lax.axis_size("tensor")
    me = lax.axis_index("tensor")
    replica = lax.axis_index("replica")
    step = 1 << apart
    far = replica + step - 2 * step * ((replica // step) % 2)
    last_rank = count - 1
    factor = FF ** (-0.5)

    barrier = pltpu.get_barrier_semaphore()
    pl.semaphore_signal(barrier, inc=1, device_id=(far, me), device_id_type=MESH)
    for hop in range(1, count):
        peer = lax.rem(me + hop, count)
        pl.semaphore_signal(barrier, inc=1, device_id=(replica, peer), device_id_type=MESH)
    pl.semaphore_wait(barrier, count)

    depth = cargo_ref.shape[0] // PIECES

    def cargo(index):
        span = pl.ds(index * depth, depth)
        return pltpu.make_async_remote_copy(
            src_ref=cargo_ref.at[span], dst_ref=landed_ref.at[span],
            send_sem=cargo_send.at[index], recv_sem=cargo_recv.at[index],
            device_id=(far, me), device_id_type=MESH,
        )

    for index in range(AHEAD):
        cargo(index).start()

    @pl.when(me == 0)
    def _():
        in_right[...] = jnp.zeros_like(in_right)

    @pl.when(me == last_rank)
    def _():
        in_left[...] = jnp.zeros_like(in_left)

    tiles, tokens = terms.shape[0], terms.shape[1]
    halves = tokens // ROWS
    chunks = tiles * halves

    def place(chunk):
        return chunk // halves, pl.ds(pl.multiple_of((chunk % halves) * ROWS, ROWS), ROWS)

    def right_copy(chunk):
        tile, rows = place(chunk)
        return pltpu.make_async_remote_copy(
            src_ref=out_right.at[tile, rows], dst_ref=in_right.at[tile, rows],
            send_sem=right_send.at[chunk], recv_sem=right_recv.at[chunk],
            device_id=(replica, lax.rem(me + 1, count)), device_id_type=MESH,
        )

    def left_copy(chunk):
        tile, rows = place(chunk)
        return pltpu.make_async_remote_copy(
            src_ref=out_left.at[tile, rows], dst_ref=in_left.at[tile, rows],
            send_sem=left_send.at[chunk], recv_sem=left_recv.at[chunk],
            device_id=(replica, lax.rem(me + count - 1, count)), device_id_type=MESH,
        )

    def turn(now, _):
        @pl.when(now < chunks)
        def _():
            tile, rows = place(now)
            columns = pl.ds(pl.multiple_of(tile * TILE, TILE), TILE)
            terms[tile, rows, :] = factor * jnp.dot(
                hidden_ref[rows, :], weight_ref[:, columns], preferred_element_type=jnp.float32
            )

        rightward = now - me

        @pl.when((rightward >= 0) & (rightward < chunks))
        def _():
            @pl.when(me > 0)
            def _():
                right_copy(rightward).wait_recv()

            @pl.when(me < last_rank)
            def _():
                tile, rows = place(rightward)
                total = terms[tile, rows, :] + in_right[tile, rows, :].astype(jnp.float32)
                out_right[tile, rows, :] = total.astype(jnp.bfloat16)
                right_copy(rightward).start()

        leftward = now - (last_rank - me)

        @pl.when((leftward >= 0) & (leftward < chunks))
        def _():
            @pl.when(me < last_rank)
            def _():
                left_copy(leftward).wait_recv()

            @pl.when(me > 0)
            def _():
                tile, rows = place(leftward)
                total = terms[tile, rows, :] + in_left[tile, rows, :].astype(jnp.float32)
                out_left[tile, rows, :] = total.astype(jnp.bfloat16)
                left_copy(leftward).start()

        if last:
            pace = (chunks + last_rank) // (BESIDE - AHEAD)
            index = AHEAD + now // pace

            @pl.when((now % pace == pace - 1) & (index < BESIDE))
            def _():
                cargo(index).start()

        return 0

    if not last:
        for index in range(AHEAD, PIECES):
            cargo(index).start()
    lax.fori_loop(0, chunks + last_rank, turn, 0)

    block = 32

    def normalise(index, _):
        rows = pl.ds(pl.multiple_of(index * block, block), block)
        outputs = jnp.concatenate(
            [
                terms[tile, rows, :]
                + in_right[tile, rows, :].astype(jnp.float32)
                + in_left[tile, rows, :].astype(jnp.float32)
                for tile in range(tiles)
            ],
            axis=1,
        )
        grad_ref[rows, :] = norm_backward(outputs, target_ref[rows, :], gain_ref[...])
        return 0

    lax.fori_loop(0, tokens // block, normalise, 0)

    if last:
        part = tokens // count
        mine = pl.ds(pl.multiple_of(me * part, part), part)
        across = pltpu.make_async_remote_copy(
            src_ref=grad_ref.at[mine], dst_ref=far_grad.at[mine],
            send_sem=grad_send, recv_sem=grad_recv,
            device_id=(far, me), device_id_type=MESH,
        )
        across.start()
        for index in range(BESIDE, PIECES):
            cargo(index).start()
        across.wait_recv()

        def share(hop):
            return pltpu.make_async_remote_copy(
                src_ref=far_grad.at[mine], dst_ref=far_grad.at[mine],
                send_sem=share_send.at[hop - 1], recv_sem=share_recv.at[hop - 1],
                device_id=(replica, lax.rem(me + hop, count)), device_id_type=MESH,
            )

        for hop in range(1, count):
            share(hop).start()
        for hop in range(1, count):
            share(hop).wait_recv()
        paired_ref[...] = far_grad[...]
        for hop in range(1, count):
            share(hop).wait_send()
        across.wait_send()

    def drain(chunk, _):
        @pl.when(me < last_rank)
        def _():
            right_copy(chunk).wait_send()

        @pl.when(me > 0)
        def _():
            left_copy(chunk).wait_send()

        return 0

    lax.fori_loop(0, chunks, drain, 0)
    for index in range(PIECES):
        cargo(index).wait()


def run_step(hidden_rows, weight_block, target_rows, norm_gain, cargo, apart, last):
    tokens, features = target_rows.shape
    tiles = features // TILE
    chunks = tiles * (tokens // ROWS)
    count = lax.axis_size("tensor")
    vmem = pl.BlockSpec(memory_space=pltpu.VMEM)
    anywhere = pl.BlockSpec(memory_space=pl.ANY)
    gradient = jax.ShapeDtypeStruct((tokens, features), jnp.bfloat16)
    landed = jax.ShapeDtypeStruct(cargo.shape, cargo.dtype)
    travelling = pltpu.VMEM((tiles, tokens, TILE), jnp.bfloat16)
    scratch = [pltpu.VMEM((tiles, tokens, TILE), jnp.float32)] + [travelling] * 4
    scratch += [pltpu.SemaphoreType.DMA((chunks,))] * 4 + [pltpu.SemaphoreType.DMA((PIECES,))] * 2
    if last:
        scratch += [pltpu.VMEM((tokens, features), jnp.bfloat16)]
        scratch += [pltpu.SemaphoreType.DMA] * 2 + [pltpu.SemaphoreType.DMA((count - 1,))] * 2
    return pl.pallas_call(
        functools.partial(step_kernel, apart, last),
        out_shape=(gradient, landed) + ((gradient,) if last else ()),
        in_specs=[vmem] * 4 + [anywhere],
        out_specs=(vmem, anywhere) + ((vmem,) if last else ()),
        scratch_shapes=scratch,
        compiler_params=pltpu.CompilerParams(
            collective_id=int(last), has_side_effects=True, vmem_limit_bytes=56 << 20
        ),
    )(hidden_rows, weight_block, target_rows, norm_gain[None], cargo)


def on_device(weights, hidden, targets, norm_gain, stragglers):
    replica_index = lax.axis_index("replica")
    weight_block = weights[0]

    def mixed(updated, paired, update_step):
        partner_index = jnp.bitwise_xor(replica_index, jnp.int32(1 << update_step))
        mask_row = stragglers[update_step]
        self_late = lax.dynamic_index_in_dim(mask_row, replica_index, keepdims=False)
        partner_late = lax.dynamic_index_in_dim(mask_row, partner_index, keepdims=False)
        keep_pair = (self_late == 0) & (partner_late == 0)
        averaged = ((updated.astype(jnp.float32) + paired.astype(jnp.float32)) * 0.5).astype(
            jnp.bfloat16
        )
        return jnp.where(keep_pair, averaged, updated)

    first, second = hidden[0, 0], hidden[0, 1]
    grad_out, paired_hidden = run_step(
        first, weight_block, targets[0, 0], norm_gain, second, 1, False
    )
    updated = descend(weight_block, first, grad_out)
    weight_block = mixed(updated, partner(updated, "replica", 0), 0)
    grad_out, paired_weight, paired_grad = run_step(
        second, weight_block, targets[0, 1], norm_gain, weight_block, 1, True
    )
    updated = descend(weight_block, second, grad_out)
    paired = descend(paired_weight, paired_hidden, paired_grad)
    return mixed(updated, paired, 1)[None]


def solution(mesh):
    placed = (
        P("replica", "tensor", None),
        P("replica", None, None, "tensor"),
        P("replica", None, None, None),
        P(),
        P(),
    )
    return jax.shard_map(
        on_device,
        mesh=mesh,
        in_specs=placed,
        out_specs=P("replica", "tensor", None),
        check_vma=False,
    )
```
